32 devices in a mesh: ctx: 16 (over z, x, core), head: 2 (over y).
Axes of the slice: x: 2, y: 2, z: 4, core: 2. Of those that a mesh axis runs over, the one named last changes fastest.
Arguments:
- queries: bfloat16 [8192, 4096], P(('ctx', 'head')), may hold values from -48 to 48
- keys: bfloat16 [8192, 4096], P(('ctx', 'head')), may hold values from -6 to 6
- values: bfloat16 [8192, 4096], P(('ctx', 'head')), may hold values from -6 to 6
- rates: float32 [8192, 8], P('ctx', 'head'), may hold values from 0.0003314563 to 0.003314563
- fast_gate: float32 [8, 512, 512], P('head'), may hold values from -0.25 to 0.25
- fast_up: float32 [8, 512, 512], P('head'), may hold values from -0.25 to 0.25
- fast_down: float32 [8, 512, 512], P('head'), may hold values from -0.25 to 0.25
- out_gain: float32 [4096], P('head'), may hold values from 0.5 to 1.5
Outputs:
- mixed: bfloat16 [8192, 4096], P('ctx', 'head')
The draws below stay inside these ranges and needn't reach their ends.
All inputs are finite; a program needn't handle non-finite values.
Results may differ from the reference program's by a relative error of at most 0.012.
Values may be sent and summed in bfloat16 or wider, within the bound.
No kernel may reach another device: no remote copies, remote signals or barrier semaphores. Data moves between devices by JAX's collectives and lax.ppermute only.
A program may use at most 192 MiB of HBM per device.

```python
import math
import jax
import jax.numpy as jnp
from jax import lax

D = 4096
AHEADS = 32
FHEADS = 8
WINDOW = 1024
AHD = 128
FD = 512
TOKENS = 8192


def drawn_pair(key):
    base = jax.random.fold_in(key, 7)
    key_query, key_key = jax.random.split(base, 2)
    query_draw = jnp.clip(2.0 * jax.random.normal(key_query, (TOKENS, D), jnp.float32), -12.0, 12.0)
    key_draw = jnp.clip(jax.random.normal(key_key, (TOKENS, D), jnp.float32), -6.0, 6.0)
    return (query_draw, key_draw)


def draw_queries(key, part):
    return drawn_pair(key)[0].astype(jnp.bfloat16)


def draw_keys(key, part):
    return drawn_pair(key)[1].astype(jnp.bfloat16)


def block_scale(stream_key, shape, cuts, least, largest):
    def one(axis_at, parts):
        heights = jax.random.uniform(jax.random.fold_in(jax.random.fold_in(stream_key, 6), axis_at), (parts,), jnp.float32, least / len(cuts), largest / len(cuts))
        return jnp.repeat(jnp.exp(heights), shape[axis_at] // parts).reshape((-1,) + (1,) * (len(shape) - axis_at - 1))

    gain = one(*cuts[0])
    for cut in cuts[1:]:
        gain = gain * one(*cut)
    return gain


def noise(key, extent, deviation, reach, pieces=(), kind=jnp.bfloat16):
    values = deviation * jax.random.normal(key, extent, jnp.float32)
    if pieces:
        values = values * block_scale(key, extent, pieces, -0.22, 0.18)
    return jnp.clip(values, -reach, reach).astype(kind)


def setup_inputs(seed: int = 0) -> dict:
    seeds = jax.random.split(jax.random.key(seed), 9)
    queries = draw_queries(jax.random.fold_in(seeds[8], 71), 0)
    keys = draw_keys(jax.random.fold_in(seeds[8], 71), 0)
    values = noise(seeds[2], (TOKENS, D), 1.0, 6.0, ((0, 32),))
    rates = jnp.clip(jnp.exp(math.log(0.003314563) - 2.3025851 * jax.random.uniform(seeds[3], (TOKENS, FHEADS), jnp.float32) ** block_scale(seeds[3], (TOKENS, FHEADS), ((0, 16), (1, 2)), -0.2, 0.2)), 0.0003314563, 0.003314563)
    fast_gate = noise(seeds[4], (FHEADS, FD, FD), FD ** -0.5, 0.25, ((0, 2),), jnp.float32)
    fast_up = noise(seeds[5], (FHEADS, FD, FD), FD ** -0.5, 0.25, ((0, 2),), jnp.float32)
    fast_down = noise(seeds[6], (FHEADS, FD, FD), FD ** -0.5, 0.25, ((0, 2),), jnp.float32)
    out_gain = jnp.clip(1.0 + 0.1 * jax.random.normal(seeds[7], (D,), jnp.float32), 0.5, 1.5)
    return dict(queries=queries, keys=keys, values=values, rates=rates, fast_gate=fast_gate, fast_up=fast_up, fast_down=fast_down, out_gain=out_gain)


epsilon = 1e-06
rms_epsilon = 1e-05

def silu_slope(pre):
    sigma = jax.nn.sigmoid(pre)
    return sigma * (1.0 + pre * (1.0 - sigma))

def column_norms(matrix):
    return jnp.sqrt(lax.optimization_barrier(jnp.sum(matrix * matrix, axis=-2)) + epsilon)

def window_attention(queries, keys, values):
    scale = 1.0 / math.sqrt(AHD)
    query_all = queries.astype(jnp.float32).reshape(TOKENS, AHEADS, AHD)
    front = jnp.zeros((WINDOW, AHEADS, AHD), jnp.float32)
    key_all = jnp.concatenate([front, keys.astype(jnp.float32).reshape(TOKENS, AHEADS, AHD)], 0)
    value_all = jnp.concatenate([front, values.astype(jnp.float32).reshape(TOKENS, AHEADS, AHD)], 0)

    def per_block(block):
        start = block * WINDOW
        query_block = lax.dynamic_slice_in_dim(query_all, start, WINDOW, 0)
        key_block = lax.dynamic_slice_in_dim(key_all, start, 2 * WINDOW, 0)
        value_block = lax.dynamic_slice_in_dim(value_all, start, 2 * WINDOW, 0)
        scores = jnp.einsum('qhd,khd->hqk', query_block, key_block) * scale
        query_pos = start + jnp.arange(WINDOW, dtype=jnp.int32)
        key_pos = start - WINDOW + jnp.arange(2 * WINDOW, dtype=jnp.int32)
        allowed = (key_pos[None, :] <= query_pos[:, None]) & (key_pos[None, :] > query_pos[:, None] - WINDOW) & (key_pos[None, :] >= 0)
        scores = jnp.where(allowed[None], scores, -1e+30)
        peak = lax.optimization_barrier(jnp.max(scores, axis=-1, keepdims=True))
        expo = jnp.exp(scores - peak)
        weights = (expo / lax.optimization_barrier(jnp.sum(expo, axis=-1, keepdims=True))).astype(jnp.bfloat16)
        return jnp.einsum('hqk,khd->qhd', weights.astype(jnp.float32), value_block)
    blocks = lax.map(per_block, jnp.arange(TOKENS // WINDOW, dtype=jnp.int32))
    return blocks.reshape(TOKENS, D)

def fast_head(inputs):
    query_rows, key_rows, value_rows, rate_col, gate_init, up_init, down_init, gain_row = inputs
    gate_cast = gate_init.astype(jnp.bfloat16)
    up_cast = up_init.astype(jnp.bfloat16)
    down_cast = down_init.astype(jnp.bfloat16)
    pre_gate = jnp.dot(key_rows, gate_cast, preferred_element_type=jnp.float32)
    pre_up = jnp.dot(key_rows, up_cast, preferred_element_type=jnp.float32)
    hidden = (jax.nn.silu(pre_gate) * pre_up).astype(jnp.bfloat16)
    target = (rate_col[:, None] * value_rows.astype(jnp.float32)).astype(jnp.bfloat16)
    step_down = jnp.dot(hidden.T, target, preferred_element_type=jnp.float32)
    back = jnp.dot(target, down_cast.T, preferred_element_type=jnp.float32)
    grad_gate = (back * pre_up * silu_slope(pre_gate)).astype(jnp.bfloat16)
    grad_up = (back * jax.nn.silu(pre_gate)).astype(jnp.bfloat16)
    step_gate = jnp.dot(key_rows.T, grad_gate, preferred_element_type=jnp.float32)
    step_up = jnp.dot(key_rows.T, grad_up, preferred_element_type=jnp.float32)
    renormed = []
    for initial, step_value in ((gate_init, step_gate), (up_init, step_up), (down_init, step_down)):
        moved = initial + step_value
        renormed.append((moved * (column_norms(initial) / column_norms(moved))[None, :]).astype(jnp.bfloat16))
    read_gate = jnp.dot(query_rows, renormed[0], preferred_element_type=jnp.float32)
    read_up = jnp.dot(query_rows, renormed[1], preferred_element_type=jnp.float32)
    read_hidden = (jax.nn.silu(read_gate) * read_up).astype(jnp.bfloat16)
    read = jnp.dot(read_hidden, renormed[2], preferred_element_type=jnp.float32)
    scale_back = lax.rsqrt(lax.optimization_barrier(jnp.mean(read * read, axis=-1, keepdims=True)) + rms_epsilon)
    return read * scale_back * gain_row[None, :]

def reference(queries, keys, values, rates, fast_gate, fast_up, fast_down, out_gain):
    attended = window_attention(queries, keys, values)

    def by_head(array):
        return array.reshape(TOKENS, FHEADS, FD).transpose(1, 0, 2)
    readout = lax.map(fast_head, (by_head(queries), by_head(keys), by_head(values), rates.T, fast_gate, fast_up, fast_down, out_gain.reshape(FHEADS, FD)))
    readout = readout.transpose(1, 0, 2).reshape(TOKENS, D)
    return (attended + readout).astype(jnp.bfloat16)
```

```python
import functools
import math

import jax
import jax.numpy as jnp
from jax import lax
from jax.experimental import pallas as pl
from jax.experimental.pallas import tpu as pltpu
from jax.sharding import Mesh, PartitionSpec as P


WINDOW = 1024
AHD = 128
FD = 512
BLOCK = 256
ROWS = 512

epsilon = 1e-06
rms_epsilon = 1e-05

f32 = jnp.float32
bf16 = jnp.bfloat16


def dot(a, b, dims):
    return lax.dot_general(a, b, (dims, ((), ())), preferred_element_type=f32)


NN = ((1,), (0,))
NT = ((1,), (1,))
TN = ((0,), (0,))

LOCAL = pl.BlockSpec(memory_space=pltpu.VMEM)


def attention_body(which, *rest, run, early, block, count):
    query_pieces, pieces = rest[:count], rest[count : 2 * count]
    early_refs = rest[2 * count : 2 * count + early]
    out_ref, query_all, key_all, value_all = rest[-4:]
    rows = query_pieces[0].shape[1]
    for over in range(count):
        source = lax.bitwise_xor(which[2], over) * rows
        query_all[pl.ds(pl.multiple_of(source, rows), rows), :] = query_pieces[over][0]
        here = pl.ds(pl.multiple_of(source + WINDOW, rows), rows)
        key_all[here, :] = pieces[over][0]
        value_all[here, :] = pieces[over][1]
    for over, early_ref in enumerate(early_refs):
        source = lax.rem(lax.bitwise_xor(which[2], over), early) * rows
        here = pl.ds(pl.multiple_of(source, rows), rows)
        key_all[here, :] = early_ref[0]
        value_all[here, :] = early_ref[1]
    q_ref = query_all.at[run * WINDOW : (run + 1) * WINDOW]
    kp_ref, vp_ref = (ref.at[run * WINDOW : (run + 1) * WINDOW] for ref in (key_all, value_all))
    kc_ref, vc_ref = (ref.at[(run + 1) * WINDOW : (run + 2) * WINDOW] for ref in (key_all, value_all))
    rows = q_ref.shape[0]
    before = kp_ref.shape[0]
    present = which[1] if early else 1
    factor = math.log2(math.e) / math.sqrt(AHD)
    bias = jnp.where(present > 0, 0.0, -1e30).astype(f32)
    own = lax.broadcasted_iota(jnp.int32, (block, block), 1) <= lax.broadcasted_iota(
        jnp.int32, (block, block), 0
    )
    for at in range(0, rows, block):
        end = at + block
        query = q_ref[at:end, :]
        score_p = dot(query, kp_ref[at:before, :], NT)
        score_c = dot(query, kc_ref[0:end, :], NT)
        pieces = [(jnp.where(own, score_c[:, at:end], score_p[:, :block] + bias), None)]
        if at + block < before:
            pieces.append((score_p[:, block:], bias))
        if at:
            pieces.append((score_c[:, :at], None))
        peak = None
        for score, shift in pieces:
            top = jnp.max(score, axis=-1, keepdims=True)
            if shift is not None:
                top = top + shift
            peak = top if peak is None else jnp.maximum(peak, top)
        peak = peak * factor
        expos = []
        total = None
        for score, shift in pieces:
            level = peak if shift is None else peak - shift
            expo = jnp.exp2(score * factor - level)
            part = jnp.sum(expo, axis=-1, keepdims=True)
            total = part if total is None else total + part
            expos.append(expo.astype(bf16))
        mixed = expos.pop(0)
        zero = jnp.zeros_like(mixed)
        result = dot(jnp.where(own, mixed, zero), vc_ref[at:end, :], NN)
        result += dot(jnp.where(own, zero, mixed), vp_ref[at:end, :], NN)
        if end < before:
            result += dot(expos.pop(0), vp_ref[end:before, :], NN)
        if at:
            result += dot(expos.pop(0), vc_ref[0:at, :], NN)
        out_ref[at:end, :] = result / total


def attention_call(which, queries, pieces, early, out, run):
    count = len(queries)
    _, rows, width = queries[0].shape
    tokens = count * rows
    heads = width // AHD
    block = min(BLOCK, WINDOW)
    pairs = heads * WINDOW * (WINDOW + block)
    given = [*queries, *pieces, *early]
    in_specs = [pl.BlockSpec((*piece.shape[:2], AHD), lambda h, _: (0, 0, h)) for piece in given]
    args = [which, *(in_hbm(piece) for piece in given)]
    aliases = {}
    if out is not None:
        in_specs.append(pl.BlockSpec(memory_space=pl.ANY))
        aliases = {len(args): 0}
        args.append(out)
    return pl.pallas_call(
        functools.partial(
            attention_body, run=run, early=len(early), block=block, count=count
        ),
        out_shape=jax.ShapeDtypeStruct((tokens, width), f32),
        grid_spec=pltpu.PrefetchScalarGridSpec(
            num_scalar_prefetch=1,
            grid=(heads,),
            in_specs=in_specs,
            out_specs=pl.BlockSpec((WINDOW, AHD), lambda h, _: (run, h)),
            scratch_shapes=[
                pltpu.VMEM((tokens, AHD), bf16),
                pltpu.VMEM((tokens + WINDOW, AHD), bf16),
                pltpu.VMEM((tokens + WINDOW, AHD), bf16),
            ],
        ),
        input_output_aliases=aliases,
        compiler_params=pltpu.CompilerParams(
            dimension_semantics=("arbitrary",), vmem_limit_bytes=40 << 20
        ),
        cost_estimate=pl.CostEstimate(
            flops=pairs * AHD * 4, transcendentals=pairs, bytes_accessed=tokens * width * 14
        ),
        name="attention",
    )(*args)


def update_body(which, rate_ref, *rest, overs, before, parts):
    count = len(overs)
    pieces, matrices = rest[:count], rest[count : count + 3]
    outs, steps = rest[count + 3 + before :], rest[-1]
    if before:
        outs = outs[:-1]
    rows = pieces[0].shape[1]
    gate, up, down = (matrix[...] for matrix in matrices)
    together = max(1, min(ROWS // rows, count))

    def joined(arrays):
        return arrays[0] if len(arrays) == 1 else jnp.concatenate(arrays, axis=0)

    for first in range(0, count, together):
        taken = range(first, min(first + together, count))
        places = [pl.multiple_of(lax.bitwise_xor(which[2], overs[at]) * rows, rows) for at in taken]
        rate = joined([rate_ref[pl.ds(at, rows), :] for at in places])
        key = joined([pieces[at][0] for at in taken])
        value = joined([pieces[at][1] for at in taken])
        pre_gate = dot(key, gate, NN)
        pre_up = dot(key, up, NN)
        target = (rate * value.astype(f32)).astype(bf16)
        back = dot(target, down, NT)
        sigma = jax.nn.sigmoid(pre_gate)
        silu = pre_gate * sigma
        hidden = (silu * pre_up).astype(bf16)
        grad_up = (back * silu).astype(bf16)
        grad_gate = (back * pre_up * (sigma * (1.0 + pre_gate * (1.0 - sigma)))).astype(bf16)
        for at, step in enumerate((dot(key, grad_gate, TN), dot(key, grad_up, TN), dot(hidden, target, TN))):
            if first:
                steps[at] += step
            elif before:
                steps[at] = rest[count + 3][at] + step
            else:
                steps[at] = step
    if parts == 1:
        outs[0][...] = steps[...]
    elif parts:
        wide = FD // parts
        for ahead, out_ref in enumerate(outs):
            at = lax.rem(which[1] + ahead, parts) * wide
            out_ref[...] = steps[:, :, pl.ds(pl.multiple_of(at, wide), wide)].astype(out_ref.dtype)


def update_call(which, overs, pieces, rate, matrices, earlier, parts):
    tokens = len(pieces) * pieces[0].shape[1]
    shape = (3, FD, FD // max(parts, 1))
    if parts:
        out_shape = [jax.ShapeDtypeStruct(shape, bf16 if ahead else f32) for ahead in range(parts)]
        scratch = [pltpu.VMEM((3, FD, FD), f32)]
    else:
        out_shape = [jax.ShapeDtypeStruct(shape, f32)]
        scratch = []
    args = [rate, *pieces, *matrices, *earlier]
    return pl.pallas_call(
        functools.partial(update_body, overs=overs, before=len(earlier), parts=parts),
        out_shape=out_shape,
        grid_spec=pltpu.PrefetchScalarGridSpec(
            num_scalar_prefetch=1,
            grid=(1,),
            in_specs=[LOCAL] * len(args),
            out_specs=[LOCAL] * len(out_shape),
            scratch_shapes=scratch,
        ),
        compiler_params=pltpu.CompilerParams(
            dimension_semantics=("arbitrary",), vmem_limit_bytes=52 << 20
        ),
        cost_estimate=pl.CostEstimate(
            flops=tokens * FD * FD * 12, transcendentals=tokens * FD, bytes_accessed=tokens * FD * 4 + FD * FD * 18
        ),
        name="update",
    )(which, *args)


def in_hbm(value):
    return pltpu.with_memory_space_constraint(value, pltpu.HBM)


def renorm_body(which, gate_ref, up_ref, down_ref, *rest):
    *got, out_ref = rest
    for at, initial_ref in enumerate((gate_ref, up_ref, down_ref)):
        initial = initial_ref[0]
        moved = initial
        for got_ref in got:
            moved = moved + got_ref[at].astype(f32)
        norm_before = jnp.sqrt(jnp.sum(initial * initial, axis=0, keepdims=True) + epsilon)
        norm_after = jnp.sqrt(jnp.sum(moved * moved, axis=0, keepdims=True) + epsilon)
        out_ref[at] = (moved * (norm_before / norm_after)).astype(bf16)


def renorm_call(which, got, gate, up, down):
    shape = got[0].shape
    wide = shape[-1]
    matrix = pl.BlockSpec((1, FD, wide), lambda i, w: (w[0], 0, w[1]))
    piece = pl.BlockSpec(shape, lambda i, w: (0, 0, 0))
    return pl.pallas_call(
        renorm_body,
        out_shape=jax.ShapeDtypeStruct(shape, bf16),
        grid_spec=pltpu.PrefetchScalarGridSpec(
            num_scalar_prefetch=1,
            grid=(1,),
            in_specs=[matrix] * 3 + [piece] * len(got),
            out_specs=piece,
        ),
        compiler_params=pltpu.CompilerParams(vmem_limit_bytes=32 << 20),
        cost_estimate=pl.CostEstimate(flops=FD * wide * 3 * 12, transcendentals=0, bytes_accessed=FD * wide * 3 * 20),
        name="renorm",
    )(which, in_hbm(gate), in_hbm(up), in_hbm(down), *got)


def readout_body(which, block, gain_ref, attended_ref, *rest, count):
    queries = rest[:count]
    *pieces, out_ref, weights = rest[count:]
    rows = queries[0].shape[1]
    wide = FD // len(pieces)
    for back, piece_ref in enumerate(pieces):
        column = lax.rem(which[1] + len(pieces) - back, len(pieces)) * wide
        weights[:, :, pl.ds(pl.multiple_of(column, wide), wide)] = piece_ref[...]
    query = queries[0][0] if count == 1 else jnp.concatenate([ref[0] for ref in queries], axis=0)
    gate = dot(query, weights[0], NN)
    up = dot(query, weights[1], NN)
    hidden = (gate * jax.nn.sigmoid(gate) * up).astype(bf16)
    read = dot(hidden, weights[2], NN)
    scale_back = lax.rsqrt(jnp.mean(read * read, axis=-1, keepdims=True) + rms_epsilon)
    readout = read * scale_back * gain_ref[...]
    for at in range(count):
        source = lax.rem(lax.bitwise_xor(which[2], at), count) * rows
        here = pl.ds(pl.multiple_of(source, rows), rows)
        out_ref[here, :] = (attended_ref[here, :] + readout[at * rows : (at + 1) * rows]).astype(bf16)


def readout_call(which, block, queries, pieces, attended, gain):
    count = len(queries)
    rows = count * queries[0].shape[1]

    def whole(array):
        return pl.BlockSpec(array.shape, lambda i, w, b: (0,) * array.ndim)

    return pl.pallas_call(
        functools.partial(readout_body, count=count),
        out_shape=jax.ShapeDtypeStruct((rows, FD), bf16),
        grid_spec=pltpu.PrefetchScalarGridSpec(
            num_scalar_prefetch=2,
            grid=(1,),
            in_specs=[whole(gain), pl.BlockSpec((rows, FD), lambda i, w, b: (b[0], 0))]
            + [whole(array) for array in (*queries, *pieces)],
            out_specs=pl.BlockSpec((rows, FD), lambda i, w, b: (0, 0)),
            scratch_shapes=[pltpu.VMEM((3, FD, FD), bf16)],
        ),
        compiler_params=pltpu.CompilerParams(
            dimension_semantics=("arbitrary",), vmem_limit_bytes=40 << 20
        ),
        cost_estimate=pl.CostEstimate(
            flops=rows * FD * FD * 6, transcendentals=rows * FD, bytes_accessed=rows * FD * 8 + FD * FD * 6
        ),
        name="readout",
    )(which, block, gain, in_hbm(attended), *queries, *pieces)


def spread_body(which, *rest, kinds, halves, subs):
    arrays, outs, sems = rest[:kinds], rest[kinds:-1], rest[-1]
    copies = []
    for over, out_ref in enumerate(outs):
        target = lax.bitwise_xor(which[2], over)
        at = pl.multiple_of((lax.rem(target, halves) * subs + lax.div(target, halves)) * FD, FD)
        for kind, array in enumerate(arrays):
            copies.append(
                pltpu.make_async_copy(array.at[:, pl.ds(at, FD)], out_ref.at[kind], sems.at[kind, over])
            )
            copies[-1].start()
    for copy in copies:
        copy.wait()


def spread_call(which, arrays, halves, subs):
    count, kinds = halves * subs, len(arrays)
    shape = (kinds, arrays[0].shape[0], FD)
    return pl.pallas_call(
        functools.partial(spread_body, kinds=kinds, halves=halves, subs=subs),
        out_shape=[jax.ShapeDtypeStruct(shape, bf16)] * count,
        grid_spec=pltpu.PrefetchScalarGridSpec(
            num_scalar_prefetch=1,
            grid=(1,),
            in_specs=[pl.BlockSpec(memory_space=pltpu.HBM)] * kinds,
            out_specs=[LOCAL] * count,
            scratch_shapes=[pltpu.SemaphoreType.DMA((kinds, count))],
        ),
        cost_estimate=pl.CostEstimate(
            flops=count * math.prod(shape), transcendentals=0, bytes_accessed=count * math.prod(shape) * 4
        ),
        name="spread",
    )(which, *arrays)


def arrange_body(which, *rest):
    *pieces, out_ref = rest
    rows = pieces[0].shape[1]
    for over, piece in enumerate(pieces):
        source = lax.bitwise_xor(which[2], over) * rows
        out_ref[:, pl.ds(pl.multiple_of(source, rows), rows), :] = piece[...]


def arrange_call(which, pieces):
    count = len(pieces)
    kinds, rows, _ = pieces[0].shape
    return pl.pallas_call(
        arrange_body,
        out_shape=jax.ShapeDtypeStruct((kinds, count * rows, FD), bf16),
        grid_spec=pltpu.PrefetchScalarGridSpec(
            num_scalar_prefetch=1,
            grid=(1,),
            in_specs=[LOCAL] * count,
            out_specs=LOCAL,
        ),
        name="arrange",
    )(which, *pieces)


def planned(queries, keys, values, rates, fast_gate, fast_up, fast_down, out_gain):
    groups, subs, halves = (lax.axis_size(axis) for axis in ("grp", "sub", "head"))
    group, sub, half = (lax.axis_index(axis) for axis in ("grp", "sub", "head"))
    rows = queries.shape[0]
    members = subs * halves
    tokens = rows * members

    place = sub * halves + half
    top = members // 2
    which = jnp.stack([sub, group, place]).astype(jnp.int32)
    order = []
    for over in range(top):
        order += [over + top] + [over + 1] * (over + 1 < top)

    def sent(piece, over):
        links = [(source, source ^ over) for source in range(members)]
        return lax.ppermute(piece, ("sub", "head"), links)

    def spread(arrays):
        return list(spread_call(which, arrays, halves, subs))

    def from_earlier(value):
        size = value.shape[0]
        reach = -(-WINDOW // size)
        pieces = []
        for distance in range(min(reach, groups - 1), 0, -1):
            count = min(size, WINDOW - (distance - 1) * size)
            links = [(source, source + distance) for source in range(groups - distance)]
            pieces.append(lax.ppermute(value[size - count :], "grp", links))
        short = WINDOW - sum(piece.shape[0] for piece in pieces)
        if short:
            pieces.insert(0, jnp.zeros((short, FD), value.dtype))
        return pieces[0] if len(pieces) == 1 else jnp.concatenate(pieces)

    def to_sub(value, over):
        return lax.ppermute(value, "sub", [(source, source ^ over) for source in range(subs)])

    def to_group(value, ahead):
        return lax.ppermute(value, "grp", [(source, (source + ahead) % groups) for source in range(groups)])

    by_sub = rates.T
    slots = []
    for over in range(subs):
        wanted = lax.dynamic_index_in_dim(by_sub, sub ^ over, 0, keepdims=False)
        slots.append(to_sub(wanted, over) if over else wanted)
    slots = jnp.stack(slots)
    rate = jnp.concatenate([lax.dynamic_index_in_dim(slots, sub ^ at, 0, keepdims=False) for at in range(subs)])
    rate = rate.reshape(tokens, 1)

    pieces = spread([keys, values])
    for over in order:
        pieces[over] = sent(pieces[over], over)
    query_pieces = spread([queries])
    for over in order:
        query_pieces[over] = sent(query_pieces[over], over)

    halved = top * rows == WINDOW
    if halved:
        links = [(source, source + 1) for source in range(groups - 1)]
        early = []
        for over in range(top):
            late = jnp.where(place >= top, pieces[over], pieces[over + top])
            early.append(lax.ppermute(late, "grp", links))

    parts = groups if FD % (groups * 128) == 0 else 1
    matrices = [
        lax.dynamic_index_in_dim(matrix, sub, 0, keepdims=False).astype(bf16)
        for matrix in (fast_gate, fast_up, fast_down)
    ]
    last = [over for over in range(members) if over % top == top - 1]
    most = [over for over in range(members) if over % top != top - 1]

    def updated(overs, earlier, parts):
        return update_call(which, overs, [pieces[over] for over in overs], rate, matrices, earlier, parts)

    begun = updated(most, [], 0)
    steps = updated(last, begun, parts)

    if parts > 1:
        got = [steps[0]] + [to_group(steps[ahead], ahead) for ahead in range(1, parts)]
        mine = renorm_call(which, got, fast_gate, fast_up, fast_down)
        weights = [mine] + [to_group(mine, ahead) for ahead in range(1, parts)]
    else:
        whole = jnp.stack([sub, sub * 0]).astype(jnp.int32)
        got = [lax.psum(steps[0], "grp") if groups > 1 else steps[0]]
        weights = [renorm_call(whole, got, fast_gate, fast_up, fast_down)]

    if halved:
        attended = attention_call(which, query_pieces, pieces, [], None, 1)
        attended = attention_call(which, query_pieces, pieces, early, attended, 0)
    else:
        key, value = arrange_call(which, pieces)
        (query,) = arrange_call(which, query_pieces)
        early_key = from_earlier(key)
        early_value = from_earlier(value)
        attended = short_attention(group, query, early_key, key, early_value, value)

    slots = [None] * subs
    gain = lax.dynamic_slice_in_dim(out_gain, sub * FD, FD).reshape(1, FD)
    for over in range(subs - 1, -1, -1):
        block = (sub ^ over).astype(jnp.int32)[None]
        chosen = query_pieces[over * halves : (over + 1) * halves]
        mixed = readout_call(which, block, chosen, weights, attended, gain)
        slots[over] = to_sub(mixed, over) if over else mixed
    if subs == 1:
        return slots[0]
    out = None
    for overs in ((0, 1), *((over,) for over in range(subs - 1, 1, -1))):
        out = join_call(which, overs, [slots[over] for over in overs], out, subs)
    return out


def join_body(which, *rest, overs):
    slots, (out_ref, sems) = rest[: len(overs)], rest[-2:]
    copies = []
    for number, over in enumerate(overs):
        at = pl.multiple_of(lax.bitwise_xor(which[0], over) * FD, FD)
        copies.append(pltpu.make_async_copy(slots[number], out_ref.at[:, pl.ds(at, FD)], sems.at[number]))
        copies[-1].start()
    for copy in copies:
        copy.wait()


def join_call(which, overs, slots, out, subs):
    raw = pl.BlockSpec(memory_space=pltpu.HBM)
    given = list(slots) if out is None else [*slots, out]
    return pl.pallas_call(
        functools.partial(join_body, overs=overs),
        out_shape=jax.ShapeDtypeStruct((slots[0].shape[0], FD * subs), bf16),
        grid_spec=pltpu.PrefetchScalarGridSpec(
            num_scalar_prefetch=1,
            grid=(1,),
            in_specs=[LOCAL] * len(slots) + [raw] * (len(given) - len(slots)),
            out_specs=raw,
            scratch_shapes=[pltpu.SemaphoreType.DMA((len(slots),))],
        ),
        input_output_aliases={} if out is None else {1 + len(slots): 0},
        name="join",
    )(which, *given)


def short_body(group_ref, q_ref, kp_ref, kc_ref, vp_ref, vc_ref, out_ref):
    rows, before = q_ref.shape[0], kp_ref.shape[0]
    factor = 1.0 / math.sqrt(AHD)
    query = q_ref[...]
    at = lax.broadcasted_iota(jnp.int32, (rows, before), 0)
    back = lax.broadcasted_iota(jnp.int32, (rows, before), 1)
    score_p = dot(query, kp_ref[...], NT) * factor
    score_p = jnp.where((back > at) & (back >= before - group_ref[0] * rows), score_p, -1e30)
    own = lax.broadcasted_iota(jnp.int32, (rows, rows), 1) <= lax.broadcasted_iota(jnp.int32, (rows, rows), 0)
    score_c = jnp.where(own, dot(query, kc_ref[...], NT) * factor, -1e30)
    peak = jnp.maximum(jnp.max(score_p, axis=-1, keepdims=True), jnp.max(score_c, axis=-1, keepdims=True))
    expo_p, expo_c = jnp.exp(score_p - peak), jnp.exp(score_c - peak)
    total = jnp.sum(expo_p, axis=-1, keepdims=True) + jnp.sum(expo_c, axis=-1, keepdims=True)
    result = dot(expo_p.astype(bf16), vp_ref[...], NN) + dot(expo_c.astype(bf16), vc_ref[...], NN)
    out_ref[...] = result / total


def short_attention(group, q, kp, kc, vp, vc):
    tokens, width = q.shape
    here = pl.BlockSpec((tokens, AHD), lambda h, _: (0, h))
    prior = pl.BlockSpec((WINDOW, AHD), lambda h, _: (0, h))
    return pl.pallas_call(
        short_body,
        out_shape=jax.ShapeDtypeStruct((tokens, width), f32),
        grid_spec=pltpu.PrefetchScalarGridSpec(
            num_scalar_prefetch=1,
            grid=(width // AHD,),
            in_specs=[here, prior, here, prior, here],
            out_specs=here,
        ),
        compiler_params=pltpu.CompilerParams(dimension_semantics=("arbitrary",), vmem_limit_bytes=40 << 20),
        name="short_attention",
    )(group.astype(jnp.int32)[None], q, kp, kc, vp, vc)


def solution(mesh):
    contexts, halves = mesh.shape["ctx"], mesh.shape["head"]

    def run(queries, keys, values, rates, fast_gate, fast_up, fast_down, out_gain):
        subs = fast_gate.shape[0] // halves
        split = Mesh(mesh.devices.reshape(contexts // subs, subs, halves), ("grp", "sub", "head"))
        rows = P(("grp", "sub", "head"), None)
        matrix = P("head", None, None)
        step = jax.shard_map(
            planned,
            mesh=split,
            in_specs=(rows, rows, rows, P(("grp", "sub"), "head"), matrix, matrix, matrix, P("head")),
            out_specs=P(("grp", "sub"), "head"),
            check_vma=False,
        )
        return step(queries, keys, values, rates, fast_gate, fast_up, fast_down, out_gain)

    return run
```

```python
import functools
import math

import jax
import jax.numpy as jnp
from jax import lax
from jax.experimental import pallas as pl
from jax.experimental.pallas import tpu as pltpu
from jax.sharding import Mesh, PartitionSpec as P


WINDOW = 1024
AHD = 128
FD = 512
BLOCK = 256
ROWS = 512

epsilon = 1e-06
rms_epsilon = 1e-05

f32 = jnp.float32
bf16 = jnp.bfloat16


def dot(a, b, dims):
    return lax.dot_general(a, b, (dims, ((), ())), preferred_element_type=f32)


NN = ((1,), (0,))
NT = ((1,), (1,))
TN = ((0,), (0,))

LOCAL = pl.BlockSpec(memory_space=pltpu.VMEM)


def attention_body(which, *rest, run, early, block, count):
    query_pieces, pieces = rest[:count], rest[count : 2 * count]
    early_refs = rest[2 * count : 2 * count + early]
    out_ref, query_all, key_all, value_all = rest[-4:]
    rows = query_pieces[0].shape[1]
    for over in range(count):
        source = lax.bitwise_xor(which[2], over) * rows
        query_all[pl.ds(pl.multiple_of(source, rows), rows), :] = query_pieces[over][0]
        here = pl.ds(pl.multiple_of(source + WINDOW, rows), rows)
        key_all[here, :] = pieces[over][0]
        value_all[here, :] = pieces[over][1]
    for over, early_ref in enumerate(early_refs):
        source = lax.rem(lax.bitwise_xor(which[2], over), early) * rows
        here = pl.ds(pl.multiple_of(source, rows), rows)
        key_all[here, :] = early_ref[0]
        value_all[here, :] = early_ref[1]
    q_ref = query_all.at[run * WINDOW : (run + 1) * WINDOW]
    kp_ref, vp_ref = (ref.at[run * WINDOW : (run + 1) * WINDOW] for ref in (key_all, value_all))
    kc_ref, vc_ref = (ref.at[(run + 1) * WINDOW : (run + 2) * WINDOW] for ref in (key_all, value_all))
    rows = q_ref.shape[0]
    before = kp_ref.shape[0]
    present = which[1] if early else 1
    factor = math.log2(math.e) / math.sqrt(AHD)
    bias = jnp.where(present > 0, 0.0, -1e30).astype(f32)
    own = lax.broadcasted_iota(jnp.int32, (block, block), 1) <= lax.broadcasted_iota(
        jnp.int32, (block, block), 0
    )
    for at in range(0, rows, block):
        end = at + block
        query = q_ref[at:end, :]
        score_p = dot(query, kp_ref[at:before, :], NT)
        score_c = dot(query, kc_ref[0:end, :], NT)
        pieces = [(jnp.where(own, score_c[:, at:end], score_p[:, :block] + bias), None)]
        if at + block < before:
            pieces.append((score_p[:, block:], bias))
        if at:
            pieces.append((score_c[:, :at], None))
        peak = None
        for score, shift in pieces:
            top = jnp.max(score, axis=-1, keepdims=True)
            if shift is not None:
                top = top + shift
            peak = top if peak is None else jnp.maximum(peak, top)
        peak = peak * factor
        expos = []
        total = None
        for score, shift in pieces:
            level = peak if shift is None else peak - shift
            expo = jnp.exp2(score * factor - level)
            part = jnp.sum(expo, axis=-1, keepdims=True)
            total = part if total is None else total + part
            expos.append(expo.astype(bf16))
        mixed = expos.pop(0)
        zero = jnp.zeros_like(mixed)
        result = dot(jnp.where(own, mixed, zero), vc_ref[at:end, :], NN)
        result += dot(jnp.where(own, zero, mixed), vp_ref[at:end, :], NN)
        if end < before:
            result += dot(expos.pop(0), vp_ref[end:before, :], NN)
        if at:
            result += dot(expos.pop(0), vc_ref[0:at, :], NN)
        out_ref[at:end, :] = result / total


def attention_call(which, queries, pieces, early, out, run):
    count = len(queries)
    _, rows, width = queries[0].shape
    tokens = count * rows
    heads = width // AHD
    block = min(BLOCK, WINDOW)
    pairs = heads * WINDOW * (WINDOW + block)
    given = [*queries, *pieces, *early]
    in_specs = [pl.BlockSpec((*piece.shape[:2], AHD), lambda h, _: (0, 0, h)) for piece in given]
    args = [which, *(in_hbm(piece) for piece in given)]
    aliases = {}
    if out is not None:
        in_specs.append(pl.BlockSpec(memory_space=pl.ANY))
        aliases = {len(args): 0}
        args.append(out)
    return pl.pallas_call(
        functools.partial(
            attention_body, run=run, early=len(early), block=block, count=count
        ),
        out_shape=jax.ShapeDtypeStruct((tokens, width), f32),
        grid_spec=pltpu.PrefetchScalarGridSpec(
            num_scalar_prefetch=1,
            grid=(heads,),
            in_specs=in_specs,
            out_specs=pl.BlockSpec((WINDOW, AHD), lambda h, _: (run, h)),
            scratch_shapes=[
                pltpu.VMEM((tokens, AHD), bf16),
                pltpu.VMEM((tokens + WINDOW, AHD), bf16),
                pltpu.VMEM((tokens + WINDOW, AHD), bf16),
            ],
        ),
        input_output_aliases=aliases,
        compiler_params=pltpu.CompilerParams(
            dimension_semantics=("arbitrary",), vmem_limit_bytes=24 << 20
        ),
        cost_estimate=pl.CostEstimate(
            flops=pairs * AHD * 4, transcendentals=pairs, bytes_accessed=tokens * width * 14
        ),
        name="attention",
    )(*args)


def update_body(which, rate_ref, *rest, overs, before, parts):
    count = len(overs)
    pieces = rest[:count]
    if before:
        sums_ref, matrices = rest[count : count + 2]
        *outs, steps, sem = rest[count + 2 :]
        sums_copy = pltpu.make_async_copy(sums_ref, steps, sem)
        sums_copy.start()
    else:
        steps, matrices = rest[count + 3 :]
        for at in range(3):
            matrices[at] = rest[count + at][0].astype(bf16)
    rows = pieces[0].shape[1]
    gate, up, down = (matrices[at] for at in range(3))
    together = max(1, min(ROWS // rows, count))

    def joined(arrays):
        return arrays[0] if len(arrays) == 1 else jnp.concatenate(arrays, axis=0)

    for first in range(0, count, together):
        taken = range(first, min(first + together, count))
        places = [pl.multiple_of(lax.bitwise_xor(which[2], overs[at]) * rows, rows) for at in taken]
        rate = joined([rate_ref[pl.ds(at, rows), :] for at in places])
        key = joined([pieces[at][0] for at in taken])
        value = joined([pieces[at][1] for at in taken])
        pre_gate = dot(key, gate, NN)
        pre_up = dot(key, up, NN)
        target = (rate * value.astype(f32)).astype(bf16)
        back = dot(target, down, NT)
        sigma = jax.nn.sigmoid(pre_gate)
        silu = pre_gate * sigma
        hidden = (silu * pre_up).astype(bf16)
        grad_up = (back * silu).astype(bf16)
        grad_gate = (back * pre_up * (sigma * (1.0 + pre_gate * (1.0 - sigma)))).astype(bf16)
        if before and not first:
            sums_copy.wait()
        for at, step in enumerate((dot(key, grad_gate, TN), dot(key, grad_up, TN), dot(hidden, target, TN))):
            if first or before:
                steps[at] += step
            else:
                steps[at] = step
    if parts == 1:
        outs[0][...] = steps[...]
    elif parts:
        wide = FD // parts
        for ahead, out_ref in enumerate(outs):
            at = lax.rem(which[1] + ahead, parts) * wide
            out_ref[...] = steps[:, :, pl.ds(pl.multiple_of(at, wide), wide)].astype(out_ref.dtype)


def update_call(which, overs, pieces, rate, given, parts):
    tokens = len(pieces) * pieces[0].shape[1]
    shape = (3, FD, FD // max(parts, 1))
    if parts:
        out_shape = [jax.ShapeDtypeStruct(shape, bf16 if ahead else f32) for ahead in range(parts)]
        scratch = [pltpu.VMEM((3, FD, FD), f32), pltpu.SemaphoreType.DMA(())]
        given_specs = [pl.BlockSpec(memory_space=pltpu.HBM), LOCAL]
    else:
        out_shape = [jax.ShapeDtypeStruct(shape, f32), jax.ShapeDtypeStruct(shape, bf16)]
        scratch = []
        given_specs = [pl.BlockSpec((1, FD, FD), lambda i, w: (w[0], 0, 0))] * 3
        given = [in_hbm(matrix) for matrix in given]
    return pl.pallas_call(
        functools.partial(update_body, overs=overs, before=bool(parts), parts=parts),
        out_shape=out_shape,
        grid_spec=pltpu.PrefetchScalarGridSpec(
            num_scalar_prefetch=1,
            grid=(1,),
            in_specs=[LOCAL] * (1 + len(pieces)) + given_specs,
            out_specs=[LOCAL] * len(out_shape),
            scratch_shapes=scratch,
        ),
        compiler_params=pltpu.CompilerParams(
            dimension_semantics=("arbitrary",), vmem_limit_bytes=30 << 20
        ),
        cost_estimate=pl.CostEstimate(
            flops=tokens * FD * FD * 12, transcendentals=tokens * FD, bytes_accessed=tokens * FD * 4 + FD * FD * 18
        ),
        name="update",
    )(which, rate, *pieces, *given)


def in_hbm(value):
    return pltpu.with_memory_space_constraint(value, pltpu.HBM)


def renorm_body(which, gate_ref, up_ref, down_ref, *rest):
    *got, out_ref = rest
    for at, initial_ref in enumerate((gate_ref, up_ref, down_ref)):
        initial = initial_ref[0]
        moved = initial
        for got_ref in got:
            moved = moved + got_ref[at].astype(f32)
        norm_before = jnp.sqrt(jnp.sum(initial * initial, axis=0, keepdims=True) + epsilon)
        norm_after = jnp.sqrt(jnp.sum(moved * moved, axis=0, keepdims=True) + epsilon)
        out_ref[at] = (moved * (norm_before / norm_after)).astype(bf16)


def renorm_call(which, got, gate, up, down):
    shape = got[0].shape
    wide = shape[-1]
    matrix = pl.BlockSpec((1, FD, wide), lambda i, w: (w[0], 0, w[1]))
    piece = pl.BlockSpec(shape, lambda i, w: (0, 0, 0))
    return pl.pallas_call(
        renorm_body,
        out_shape=jax.ShapeDtypeStruct(shape, bf16),
        grid_spec=pltpu.PrefetchScalarGridSpec(
            num_scalar_prefetch=1,
            grid=(1,),
            in_specs=[matrix] * 3 + [piece] * len(got),
            out_specs=piece,
        ),
        compiler_params=pltpu.CompilerParams(vmem_limit_bytes=16 << 20),
        cost_estimate=pl.CostEstimate(flops=FD * wide * 3 * 12, transcendentals=0, bytes_accessed=FD * wide * 3 * 20),
        name="renorm",
    )(which, in_hbm(gate), in_hbm(up), in_hbm(down), *got)


def readout_body(which, block, gain_ref, attended_ref, *rest, count):
    queries = rest[:count]
    *pieces, out_ref, weights = rest[count:]
    rows = queries[0].shape[1]
    wide = FD // len(pieces)
    for back, piece_ref in enumerate(pieces):
        column = lax.rem(which[1] + len(pieces) - back, len(pieces)) * wide
        weights[:, :, pl.ds(pl.multiple_of(column, wide), wide)] = piece_ref[...]
    query = queries[0][0] if count == 1 else jnp.concatenate([ref[0] for ref in queries], axis=0)
    gate = dot(query, weights[0], NN)
    up = dot(query, weights[1], NN)
    hidden = (gate * jax.nn.sigmoid(gate) * up).astype(bf16)
    read = dot(hidden, weights[2], NN)
    scale_back = lax.rsqrt(jnp.mean(read * read, axis=-1, keepdims=True) + rms_epsilon)
    readout = read * scale_back * gain_ref[...]
    for at in range(count):
        source = lax.rem(lax.bitwise_xor(which[2], at), count) * rows
        here = pl.ds(pl.multiple_of(source, rows), rows)
        out_ref[here, :] = (attended_ref[here, :] + readout[at * rows : (at + 1) * rows]).astype(bf16)


def readout_call(which, block, queries, pieces, attended, gain):
    count = len(queries)
    rows = count * queries[0].shape[1]

    def whole(array):
        return pl.BlockSpec(array.shape, lambda i, w, b: (0,) * array.ndim)

    return pl.pallas_call(
        functools.partial(readout_body, count=count),
        out_shape=jax.ShapeDtypeStruct((rows, FD), bf16),
        grid_spec=pltpu.PrefetchScalarGridSpec(
            num_scalar_prefetch=2,
            grid=(1,),
            in_specs=[whole(gain), pl.BlockSpec((rows, FD), lambda i, w, b: (b[0], 0))]
            + [whole(array) for array in (*queries, *pieces)],
            out_specs=pl.BlockSpec((rows, FD), lambda i, w, b: (0, 0)),
            scratch_shapes=[pltpu.VMEM((3, FD, FD), bf16)],
        ),
        compiler_params=pltpu.CompilerParams(
            dimension_semantics=("arbitrary",), vmem_limit_bytes=16 << 20
        ),
        cost_estimate=pl.CostEstimate(
            flops=rows * FD * FD * 6, transcendentals=rows * FD, bytes_accessed=rows * FD * 8 + FD * FD * 6
        ),
        name="readout",
    )(which, block, gain, attended, *queries, *pieces)


def spread_body(which, *rest, overs, kinds, halves, subs):
    arrays, outs, sems = rest[:kinds], rest[kinds:-1], rest[-1]
    copies = []
    for number, (over, out_ref) in enumerate(zip(overs, outs)):
        target = lax.bitwise_xor(which[2], over)
        at = pl.multiple_of((lax.rem(target, halves) * subs + lax.div(target, halves)) * FD, FD)
        for kind, array in enumerate(arrays):
            copies.append(
                pltpu.make_async_copy(array.at[:, pl.ds(at, FD)], out_ref.at[kind], sems.at[kind, number])
            )
            copies[-1].start()
    for copy in copies:
        copy.wait()


def spread_call(which, arrays, overs, halves, subs):
    count, kinds = len(overs), len(arrays)
    shape = (kinds, arrays[0].shape[0], FD)
    return pl.pallas_call(
        functools.partial(spread_body, overs=overs, kinds=kinds, halves=halves, subs=subs),
        out_shape=[jax.ShapeDtypeStruct(shape, bf16)] * count,
        grid_spec=pltpu.PrefetchScalarGridSpec(
            num_scalar_prefetch=1,
            grid=(1,),
            in_specs=[pl.BlockSpec(memory_space=pltpu.HBM)] * kinds,
            out_specs=[LOCAL] * count,
            scratch_shapes=[pltpu.SemaphoreType.DMA((kinds, count))],
        ),
        compiler_params=pltpu.CompilerParams(vmem_limit_bytes=12 << 20),
        cost_estimate=pl.CostEstimate(
            flops=count * math.prod(shape), transcendentals=0, bytes_accessed=count * math.prod(shape) * 4
        ),
        name="spread",
    )(which, *(in_hbm(array) for array in arrays))


def arrange_body(which, *rest):
    *pieces, out_ref = rest
    rows = pieces[0].shape[1]
    for over, piece in enumerate(pieces):
        source = lax.bitwise_xor(which[2], over) * rows
        out_ref[:, pl.ds(pl.multiple_of(source, rows), rows), :] = piece[...]


def arrange_call(which, pieces):
    count = len(pieces)
    kinds, rows, _ = pieces[0].shape
    return pl.pallas_call(
        arrange_body,
        out_shape=jax.ShapeDtypeStruct((kinds, count * rows, FD), bf16),
        grid_spec=pltpu.PrefetchScalarGridSpec(
            num_scalar_prefetch=1,
            grid=(1,),
            in_specs=[LOCAL] * count,
            out_specs=LOCAL,
        ),
        name="arrange",
    )(which, *pieces)


def planned(queries, keys, values, rates, fast_gate, fast_up, fast_down, out_gain):
    groups, subs, halves = (lax.axis_size(axis) for axis in ("grp", "sub", "head"))
    group, sub, half = (lax.axis_index(axis) for axis in ("grp", "sub", "head"))
    rows = queries.shape[0]
    members = subs * halves
    tokens = rows * members

    place = sub * halves + half
    top = members // 2
    which = jnp.stack([sub, group, place]).astype(jnp.int32)
    order = []
    for over in range(top):
        order += [over + top] + [over + 1] * (over + 1 < top)

    def sent(piece, over):
        links = [(source, source ^ over) for source in range(members)]
        return lax.ppermute(piece, ("sub", "head"), links)

    def spread(arrays, calls):
        result = [None] * members
        for call in range(calls):
            overs = [over for over in range(members) if over % top * calls // top == call]
            for over, piece in zip(overs, spread_call(which, arrays, overs, halves, subs)):
                result[over] = piece
        return result

    def from_earlier(value):
        size = value.shape[0]
        reach = -(-WINDOW // size)
        pieces = []
        for distance in range(min(reach, groups - 1), 0, -1):
            count = min(size, WINDOW - (distance - 1) * size)
            links = [(source, source + distance) for source in range(groups - distance)]
            pieces.append(lax.ppermute(value[size - count :], "grp", links))
        short = WINDOW - sum(piece.shape[0] for piece in pieces)
        if short:
            pieces.insert(0, jnp.zeros((short, FD), value.dtype))
        return pieces[0] if len(pieces) == 1 else jnp.concatenate(pieces)

    def to_sub(value, over):
        return lax.ppermute(value, "sub", [(source, source ^ over) for source in range(subs)])

    def to_group(value, ahead):
        return lax.ppermute(value, "grp", [(source, (source + ahead) % groups) for source in range(groups)])

    by_sub = rates.T
    slots = []
    for over in range(subs):
        wanted = lax.dynamic_index_in_dim(by_sub, sub ^ over, 0, keepdims=False)
        slots.append(to_sub(wanted, over) if over else wanted)
    slots = jnp.stack(slots)
    rate = jnp.concatenate([lax.dynamic_index_in_dim(slots, sub ^ at, 0, keepdims=False) for at in range(subs)])
    rate = rate.reshape(tokens, 1)

    pieces = spread([keys, values], top)
    for over in order:
        pieces[over] = sent(pieces[over], over)
    query_pieces = spread([queries], 1)
    for over in order:
        query_pieces[over] = sent(query_pieces[over], over)

    halved = top * rows == WINDOW
    if halved:
        links = [(source, source + 1) for source in range(groups - 1)]
        early = []
        for over in range(top):
            late = jnp.where(place >= top, pieces[over], pieces[over + top])
            early.append(lax.ppermute(late, "grp", links))

    parts = groups if FD % (groups * 128) == 0 else 1
    last = [over for over in range(members) if over % top == top - 1]
    most = [over for over in range(members) if over % top != top - 1]

    def updated(overs, given, parts):
        return update_call(which, overs, [pieces[over] for over in overs], rate, given, parts)

    begun = updated(most, (fast_gate, fast_up, fast_down), 0)
    steps = updated(last, begun, parts)

    if parts > 1:
        got = [steps[0]] + [to_group(steps[ahead], ahead) for ahead in range(1, parts)]
        mine = renorm_call(which, got, fast_gate, fast_up, fast_down)
        weights = [mine] + [to_group(mine, ahead) for ahead in range(1, parts)]
    else:
        whole = jnp.stack([sub, sub * 0]).astype(jnp.int32)
        got = [lax.psum(steps[0], "grp") if groups > 1 else steps[0]]
        weights = [renorm_call(whole, got, fast_gate, fast_up, fast_down)]

    if halved:
        attended = attention_call(which, query_pieces, pieces, [], None, 1)
        attended = attention_call(which, query_pieces, pieces, early, attended, 0)
    else:
        key, value = arrange_call(which, pieces)
        (query,) = arrange_call(which, query_pieces)
        early_key = from_earlier(key)
        early_value = from_earlier(value)
        attended = short_attention(group, query, early_key, key, early_value, value)

    slots = [None] * subs
    gain = lax.dynamic_slice_in_dim(out_gain, sub * FD, FD).reshape(1, FD)
    for over in range(subs - 1, -1, -1):
        block = (sub ^ over).astype(jnp.int32)[None]
        chosen = query_pieces[over * halves : (over + 1) * halves]
        mixed = readout_call(which, block, chosen, weights, attended, gain)
        slots[over] = to_sub(mixed, over) if over else mixed
    if subs == 1:
        return slots[0]
    out = None
    for overs in ((0, 1), *((over,) for over in range(subs - 1, 1, -1))):
        out = join_call(which, overs, [slots[over] for over in overs], out, subs)
    return out


def join_body(which, *rest, overs):
    slots, (out_ref, sems) = rest[: len(overs)], rest[-2:]
    copies = []
    for number, over in enumerate(overs):
        at = pl.multiple_of(lax.bitwise_xor(which[0], over) * FD, FD)
        copies.append(pltpu.make_async_copy(slots[number], out_ref.at[:, pl.ds(at, FD)], sems.at[number]))
        copies[-1].start()
    for copy in copies:
        copy.wait()


def join_call(which, overs, slots, out, subs):
    raw = pl.BlockSpec(memory_space=pltpu.HBM)
    given = list(slots) if out is None else [*slots, out]
    return pl.pallas_call(
        functools.partial(join_body, overs=overs),
        out_shape=jax.ShapeDtypeStruct((slots[0].shape[0], FD * subs), bf16),
        grid_spec=pltpu.PrefetchScalarGridSpec(
            num_scalar_prefetch=1,
            grid=(1,),
            in_specs=[LOCAL] * len(slots) + [raw] * (len(given) - len(slots)),
            out_specs=raw,
            scratch_shapes=[pltpu.SemaphoreType.DMA((len(slots),))],
        ),
        input_output_aliases={} if out is None else {1 + len(slots): 0},
        compiler_params=pltpu.CompilerParams(vmem_limit_bytes=6 << 20),
        name="join",
    )(which, *given)


def short_body(group_ref, q_ref, kp_ref, kc_ref, vp_ref, vc_ref, out_ref):
    rows, before = q_ref.shape[0], kp_ref.shape[0]
    factor = 1.0 / math.sqrt(AHD)
    query = q_ref[...]
    at = lax.broadcasted_iota(jnp.int32, (rows, before), 0)
    back = lax.broadcasted_iota(jnp.int32, (rows, before), 1)
    score_p = dot(query, kp_ref[...], NT) * factor
    score_p = jnp.where((back > at) & (back >= before - group_ref[0] * rows), score_p, -1e30)
    own = lax.broadcasted_iota(jnp.int32, (rows, rows), 1) <= lax.broadcasted_iota(jnp.int32, (rows, rows), 0)
    score_c = jnp.where(own, dot(query, kc_ref[...], NT) * factor, -1e30)
    peak = jnp.maximum(jnp.max(score_p, axis=-1, keepdims=True), jnp.max(score_c, axis=-1, keepdims=True))
    expo_p, expo_c = jnp.exp(score_p - peak), jnp.exp(score_c - peak)
    total = jnp.sum(expo_p, axis=-1, keepdims=True) + jnp.sum(expo_c, axis=-1, keepdims=True)
    result = dot(expo_p.astype(bf16), vp_ref[...], NN) + dot(expo_c.astype(bf16), vc_ref[...], NN)
    out_ref[...] = result / total


def short_attention(group, q, kp, kc, vp, vc):
    tokens, width = q.shape
    here = pl.BlockSpec((tokens, AHD), lambda h, _: (0, h))
    prior = pl.BlockSpec((WINDOW, AHD), lambda h, _: (0, h))
    return pl.pallas_call(
        short_body,
        out_shape=jax.ShapeDtypeStruct((tokens, width), f32),
        grid_spec=pltpu.PrefetchScalarGridSpec(
            num_scalar_prefetch=1,
            grid=(width // AHD,),
            in_specs=[here, prior, here, prior, here],
            out_specs=here,
        ),
        compiler_params=pltpu.CompilerParams(dimension_semantics=("arbitrary",), vmem_limit_bytes=40 << 20),
        name="short_attention",
    )(group.astype(jnp.int32)[None], q, kp, kc, vp, vc)


def solution(mesh):
    contexts, halves = mesh.shape["ctx"], mesh.shape["head"]

    def run(queries, keys, values, rates, fast_gate, fast_up, fast_down, out_gain):
        subs = fast_gate.shape[0] // halves
        split = Mesh(mesh.devices.reshape(contexts // subs, subs, halves), ("grp", "sub", "head"))
        rows = P(("grp", "sub", "head"), None)
        matrix = P("head", None, None)
        step = jax.shard_map(
            planned,
            mesh=split,
            in_specs=(rows, rows, rows, P(("grp", "sub"), "head"), matrix, matrix, matrix, P("head")),
            out_specs=P(("grp", "sub"), "head"),
            check_vma=False,
        )
        return step(queries, keys, values, rates, fast_gate, fast_up, fast_down, out_gain)

    return run
```

```python
import functools
import math

import jax
import jax.numpy as jnp
from jax import lax
from jax.experimental import pallas as pl
from jax.experimental.pallas import tpu as pltpu
from jax.sharding import Mesh, PartitionSpec as P


WINDOW = 1024
AHD = 128
FD = 512
BLOCK = 256
ROWS = 512

epsilon = 1e-06
rms_epsilon = 1e-05

f32 = jnp.float32
bf16 = jnp.bfloat16


def dot(a, b, dims):
    return lax.dot_general(a, b, (dims, ((), ())), preferred_element_type=f32)


NN = ((1,), (0,))
NT = ((1,), (1,))
TN = ((0,), (0,))

LOCAL = pl.BlockSpec(memory_space=pltpu.VMEM)

SHARES = ((0, 2), (2, 3))


def attention_body(which, *rest, run, early, block, count):
    query_pieces, pieces = rest[:count], rest[count : 2 * count]
    early_refs = rest[2 * count : 2 * count + early]
    out_ref, query_all, key_all, value_all = rest[-4:]
    rows = query_pieces[0].shape[1]
    for over in range(count):
        source = lax.bitwise_xor(which[2], over) * rows
        query_all[pl.ds(pl.multiple_of(source, rows), rows), :] = query_pieces[over][0]
        here = pl.ds(pl.multiple_of(source + WINDOW, rows), rows)
        key_all[here, :] = pieces[over][0]
        value_all[here, :] = pieces[over][1]
    for over, early_ref in enumerate(early_refs):
        source = lax.rem(lax.bitwise_xor(which[2], over), early) * rows
        here = pl.ds(pl.multiple_of(source, rows), rows)
        key_all[here, :] = early_ref[0]
        value_all[here, :] = early_ref[1]
    q_ref = query_all.at[run * WINDOW : (run + 1) * WINDOW]
    kp_ref, vp_ref = (ref.at[run * WINDOW : (run + 1) * WINDOW] for ref in (key_all, value_all))
    kc_ref, vc_ref = (ref.at[(run + 1) * WINDOW : (run + 2) * WINDOW] for ref in (key_all, value_all))
    rows = q_ref.shape[0]
    before = kp_ref.shape[0]
    present = which[1] if early else 1
    factor = math.log2(math.e) / math.sqrt(AHD)
    bias = jnp.where(present > 0, 0.0, -1e30).astype(f32)
    own = lax.broadcasted_iota(jnp.int32, (block, block), 1) <= lax.broadcasted_iota(
        jnp.int32, (block, block), 0
    )
    for at in range(0, rows, block):
        end = at + block
        query = q_ref[at:end, :]
        score_p = dot(query, kp_ref[at:before, :], NT)
        score_c = dot(query, kc_ref[0:end, :], NT)
        pieces = [(jnp.where(own, score_c[:, at:end], score_p[:, :block] + bias), None)]
        if at + block < before:
            pieces.append((score_p[:, block:], bias))
        if at:
            pieces.append((score_c[:, :at], None))
        peak = None
        for score, shift in pieces:
            top = jnp.max(score, axis=-1, keepdims=True)
            if shift is not None:
                top = top + shift
            peak = top if peak is None else jnp.maximum(peak, top)
        peak = peak * factor
        expos = []
        total = None
        for score, shift in pieces:
            level = peak if shift is None else peak - shift
            expo = jnp.exp2(score * factor - level)
            part = jnp.sum(expo, axis=-1, keepdims=True)
            total = part if total is None else total + part
            expos.append(expo.astype(bf16))
        mixed = expos.pop(0)
        zero = jnp.zeros_like(mixed)
        result = dot(jnp.where(own, mixed, zero), vc_ref[at:end, :], NN)
        result += dot(jnp.where(own, zero, mixed), vp_ref[at:end, :], NN)
        if end < before:
            result += dot(expos.pop(0), vp_ref[end:before, :], NN)
        if at:
            result += dot(expos.pop(0), vc_ref[0:at, :], NN)
        out_ref[at:end, :] = result / total


def attention_call(which, queries, pieces, early, out, run):
    count = len(queries)
    _, rows, width = queries[0].shape
    tokens = count * rows
    heads = width // AHD
    block = min(BLOCK, WINDOW)
    pairs = heads * WINDOW * (WINDOW + block)
    given = [*queries, *pieces, *early]
    in_specs = [pl.BlockSpec((*piece.shape[:2], AHD), lambda h, _: (0, 0, h)) for piece in given]
    args = [which, *(in_hbm(piece) for piece in given)]
    aliases = {}
    if out is not None:
        in_specs.append(pl.BlockSpec(memory_space=pl.ANY))
        aliases = {len(args): 0}
        args.append(out)
    return pl.pallas_call(
        functools.partial(
            attention_body, run=run, early=len(early), block=block, count=count
        ),
        out_shape=jax.ShapeDtypeStruct((tokens, width), f32),
        grid_spec=pltpu.PrefetchScalarGridSpec(
            num_scalar_prefetch=1,
            grid=(heads,),
            in_specs=in_specs,
            out_specs=pl.BlockSpec((WINDOW, AHD), lambda h, _: (run, h)),
            scratch_shapes=[
                pltpu.VMEM((tokens, AHD), bf16),
                pltpu.VMEM((tokens + WINDOW, AHD), bf16),
                pltpu.VMEM((tokens + WINDOW, AHD), bf16),
            ],
        ),
        input_output_aliases=aliases,
        compiler_params=pltpu.CompilerParams(
            dimension_semantics=("arbitrary",), vmem_limit_bytes=24 << 20
        ),
        cost_estimate=pl.CostEstimate(
            flops=pairs * AHD * 4, transcendentals=pairs, bytes_accessed=tokens * width * 14
        ),
        name="attention",
    )(*args)


def update_body(which, rate_ref, *rest, overs, before, parts):
    count = len(overs)
    pieces = rest[:count]
    if before:
        sums_ref, matrices = rest[count : count + 2]
        *outs, steps, sem = rest[count + 2 :]
        sums_copy = pltpu.make_async_copy(sums_ref, steps, sem)
        sums_copy.start()
    else:
        steps, matrices = rest[count + 3 :]
        for at in range(3):
            matrices[at] = rest[count + at][0].astype(bf16)
    rows = pieces[0].shape[1]
    gate, up, down = (matrices[at] for at in range(3))
    together = max(1, min(ROWS // rows, count))

    def joined(arrays):
        return arrays[0] if len(arrays) == 1 else jnp.concatenate(arrays, axis=0)

    for first in range(0, count, together):
        taken = range(first, min(first + together, count))
        places = [pl.multiple_of(lax.bitwise_xor(which[2], overs[at]) * rows, rows) for at in taken]
        rate = joined([rate_ref[pl.ds(at, rows), :] for at in places])
        key = joined([pieces[at][0] for at in taken])
        value = joined([pieces[at][1] for at in taken])
        pre_gate = dot(key, gate, NN)
        pre_up = dot(key, up, NN)
        target = (rate * value.astype(f32)).astype(bf16)
        back = dot(target, down, NT)
        sigma = jax.nn.sigmoid(pre_gate)
        silu = pre_gate * sigma
        hidden = (silu * pre_up).astype(bf16)
        grad_up = (back * silu).astype(bf16)
        grad_gate = (back * pre_up * (sigma * (1.0 + pre_gate * (1.0 - sigma)))).astype(bf16)
        if before and not first:
            sums_copy.wait()
        for at, step in enumerate((dot(key, grad_gate, TN), dot(key, grad_up, TN), dot(hidden, target, TN))):
            if first or before:
                steps[at] += step
            else:
                steps[at] = step
    if parts == 1:
        outs[0][...] = steps[...]
    elif parts:
        wide = FD // parts
        for number, (low, high) in enumerate(SHARES):
            for ahead in range(parts):
                out_ref = outs[number * parts + ahead]
                at = lax.rem(which[1] + ahead, parts) * wide
                out_ref[...] = steps[low:high, :, pl.ds(pl.multiple_of(at, wide), wide)].astype(out_ref.dtype)


def update_call(which, overs, pieces, rate, given, parts):
    tokens = len(pieces) * pieces[0].shape[1]
    shape = (3, FD, FD // max(parts, 1))
    if parts > 1:
        out_shape = [
            jax.ShapeDtypeStruct((high - low, *shape[1:]), bf16 if ahead else f32)
            for low, high in SHARES
            for ahead in range(parts)
        ]
    elif parts:
        out_shape = [jax.ShapeDtypeStruct(shape, f32)]
    if parts:
        scratch = [pltpu.VMEM((3, FD, FD), f32), pltpu.SemaphoreType.DMA(())]
        given_specs = [pl.BlockSpec(memory_space=pltpu.HBM), LOCAL]
    else:
        out_shape = [jax.ShapeDtypeStruct(shape, f32), jax.ShapeDtypeStruct(shape, bf16)]
        scratch = []
        given_specs = [pl.BlockSpec((1, FD, FD), lambda i, w: (w[0], 0, 0))] * 3
        given = [in_hbm(matrix) for matrix in given]
    return pl.pallas_call(
        functools.partial(update_body, overs=overs, before=bool(parts), parts=parts),
        out_shape=out_shape,
        grid_spec=pltpu.PrefetchScalarGridSpec(
            num_scalar_prefetch=1,
            grid=(1,),
            in_specs=[LOCAL] * (1 + len(pieces)) + given_specs,
            out_specs=[LOCAL] * len(out_shape),
            scratch_shapes=scratch,
        ),
        compiler_params=pltpu.CompilerParams(
            dimension_semantics=("arbitrary",), vmem_limit_bytes=30 << 20
        ),
        cost_estimate=pl.CostEstimate(
            flops=tokens * FD * FD * 12, transcendentals=tokens * FD, bytes_accessed=tokens * FD * 4 + FD * FD * 18
        ),
        name="update",
    )(which, rate, *pieces, *given)


def in_hbm(value):
    return pltpu.with_memory_space_constraint(value, pltpu.HBM)


def renorm_body(which, *rest):
    *refs, out_ref = rest
    count = out_ref.shape[0]
    for at, initial_ref in enumerate(refs[:count]):
        initial = initial_ref[0]
        moved = initial
        for got_ref in refs[count:]:
            moved = moved + got_ref[at].astype(f32)
        norm_before = jnp.sqrt(jnp.sum(initial * initial, axis=0, keepdims=True) + epsilon)
        norm_after = jnp.sqrt(jnp.sum(moved * moved, axis=0, keepdims=True) + epsilon)
        out_ref[at] = (moved * (norm_before / norm_after)).astype(bf16)


def renorm_call(which, got, matrices):
    shape = got[0].shape
    wide = shape[-1]
    matrix = pl.BlockSpec((1, FD, wide), lambda i, w: (w[0], 0, w[1]))
    piece = pl.BlockSpec(shape, lambda i, w: (0, 0, 0))
    return pl.pallas_call(
        renorm_body,
        out_shape=jax.ShapeDtypeStruct(shape, bf16),
        grid_spec=pltpu.PrefetchScalarGridSpec(
            num_scalar_prefetch=1,
            grid=(1,),
            in_specs=[matrix] * len(matrices) + [piece] * len(got),
            out_specs=piece,
        ),
        compiler_params=pltpu.CompilerParams(vmem_limit_bytes=16 << 20),
        cost_estimate=pl.CostEstimate(flops=FD * wide * 3 * 12, transcendentals=0, bytes_accessed=FD * wide * 3 * 20),
        name="renorm",
    )(which, *(in_hbm(matrix) for matrix in matrices), *got)


def readout_body(which, block, gain_ref, attended_ref, *rest, count, shares):
    queries = rest[:count]
    *pieces, out_ref, weights = rest[count:]
    rows = queries[0].shape[1]
    parts = len(pieces) // shares
    wide = FD // parts
    low = 0
    for number in range(shares):
        high = low + pieces[number * parts].shape[0]
        for back in range(parts):
            column = lax.rem(which[1] + parts - back, parts) * wide
            weights[low:high, :, pl.ds(pl.multiple_of(column, wide), wide)] = pieces[number * parts + back][...]
        low = high
    query = queries[0][0] if count == 1 else jnp.concatenate([ref[0] for ref in queries], axis=0)
    gate = dot(query, weights[0], NN)
    up = dot(query, weights[1], NN)
    hidden = (gate * jax.nn.sigmoid(gate) * up).astype(bf16)
    read = dot(hidden, weights[2], NN)
    scale_back = lax.rsqrt(jnp.mean(read * read, axis=-1, keepdims=True) + rms_epsilon)
    readout = read * scale_back * gain_ref[...]
    for at in range(count):
        source = lax.rem(lax.bitwise_xor(which[2], at), count) * rows
        here = pl.ds(pl.multiple_of(source, rows), rows)
        out_ref[here, :] = (attended_ref[here, :] + readout[at * rows : (at + 1) * rows]).astype(bf16)


def readout_call(which, block, queries, weights, attended, gain):
    count = len(queries)
    pieces = [piece for share in weights for piece in share]
    rows = count * queries[0].shape[1]

    def whole(array):
        return pl.BlockSpec(array.shape, lambda i, w, b: (0,) * array.ndim)

    return pl.pallas_call(
        functools.partial(readout_body, count=count, shares=len(weights)),
        out_shape=jax.ShapeDtypeStruct((rows, FD), bf16),
        grid_spec=pltpu.PrefetchScalarGridSpec(
            num_scalar_prefetch=2,
            grid=(1,),
            in_specs=[whole(gain), pl.BlockSpec((rows, FD), lambda i, w, b: (b[0], 0))]
            + [whole(array) for array in (*queries, *pieces)],
            out_specs=pl.BlockSpec((rows, FD), lambda i, w, b: (0, 0)),
            scratch_shapes=[pltpu.VMEM((3, FD, FD), bf16)],
        ),
        compiler_params=pltpu.CompilerParams(
            dimension_semantics=("arbitrary",), vmem_limit_bytes=16 << 20
        ),
        cost_estimate=pl.CostEstimate(
            flops=rows * FD * FD * 6, transcendentals=rows * FD, bytes_accessed=rows * FD * 8 + FD * FD * 6
        ),
        name="readout",
    )(which, block, gain, attended, *queries, *pieces)


def spread_body(which, *rest, overs, kinds, halves, subs):
    arrays, outs, sems = rest[:kinds], rest[kinds:-1], rest[-1]
    copies = []
    for number, (over, out_ref) in enumerate(zip(overs, outs)):
        target = lax.bitwise_xor(which[2], over)
        at = pl.multiple_of((lax.rem(target, halves) * subs + lax.div(target, halves)) * FD, FD)
        for kind, array in enumerate(arrays):
            copies.append(
                pltpu.make_async_copy(array.at[:, pl.ds(at, FD)], out_ref.at[kind], sems.at[kind, number])
            )
            copies[-1].start()
    for copy in copies:
        copy.wait()


def spread_call(which, arrays, overs, halves, subs):
    count, kinds = len(overs), len(arrays)
    shape = (kinds, arrays[0].shape[0], FD)
    return pl.pallas_call(
        functools.partial(spread_body, overs=overs, kinds=kinds, halves=halves, subs=subs),
        out_shape=[jax.ShapeDtypeStruct(shape, bf16)] * count,
        grid_spec=pltpu.PrefetchScalarGridSpec(
            num_scalar_prefetch=1,
            grid=(1,),
            in_specs=[pl.BlockSpec(memory_space=pltpu.HBM)] * kinds,
            out_specs=[LOCAL] * count,
            scratch_shapes=[pltpu.SemaphoreType.DMA((kinds, count))],
        ),
        compiler_params=pltpu.CompilerParams(vmem_limit_bytes=12 << 20),
        cost_estimate=pl.CostEstimate(
            flops=count * math.prod(shape), transcendentals=0, bytes_accessed=count * math.prod(shape) * 4
        ),
        name="spread",
    )(which, *(in_hbm(array) for array in arrays))


def arrange_body(which, *rest):
    *pieces, out_ref = rest
    rows = pieces[0].shape[1]
    for over, piece in enumerate(pieces):
        source = lax.bitwise_xor(which[2], over) * rows
        out_ref[:, pl.ds(pl.multiple_of(source, rows), rows), :] = piece[...]


def arrange_call(which, pieces):
    count = len(pieces)
    kinds, rows, _ = pieces[0].shape
    return pl.pallas_call(
        arrange_body,
        out_shape=jax.ShapeDtypeStruct((kinds, count * rows, FD), bf16),
        grid_spec=pltpu.PrefetchScalarGridSpec(
            num_scalar_prefetch=1,
            grid=(1,),
            in_specs=[LOCAL] * count,
            out_specs=LOCAL,
        ),
        name="arrange",
    )(which, *pieces)


def planned(queries, keys, values, rates, fast_gate, fast_up, fast_down, out_gain):
    groups, subs, halves = (lax.axis_size(axis) for axis in ("grp", "sub", "head"))
    group, sub, half = (lax.axis_index(axis) for axis in ("grp", "sub", "head"))
    rows = queries.shape[0]
    members = subs * halves
    tokens = rows * members

    place = sub * halves + half
    top = members // 2
    which = jnp.stack([sub, group, place]).astype(jnp.int32)
    order = []
    for over in range(top):
        order += [over + top] + [over + 1] * (over + 1 < top)

    def sent(piece, over):
        links = [(source, source ^ over) for source in range(members)]
        return lax.ppermute(piece, ("sub", "head"), links)

    def spread(arrays, calls):
        result = [None] * members
        for call in range(calls):
            overs = [over for over in range(members) if over % top * calls // top == call]
            if calls > 1 and call < 2:
                overs = [1 - call, top + call]
            for over, piece in zip(overs, spread_call(which, arrays, overs, halves, subs)):
                result[over] = piece
        return result

    def from_earlier(value):
        size = value.shape[0]
        reach = -(-WINDOW // size)
        pieces = []
        for distance in range(min(reach, groups - 1), 0, -1):
            count = min(size, WINDOW - (distance - 1) * size)
            links = [(source, source + distance) for source in range(groups - distance)]
            pieces.append(lax.ppermute(value[size - count :], "grp", links))
        short = WINDOW - sum(piece.shape[0] for piece in pieces)
        if short:
            pieces.insert(0, jnp.zeros((short, FD), value.dtype))
        return pieces[0] if len(pieces) == 1 else jnp.concatenate(pieces)

    def to_sub(value, over):
        return lax.ppermute(value, "sub", [(source, source ^ over) for source in range(subs)])

    def to_group(value, ahead):
        return lax.ppermute(value, "grp", [(source, (source + ahead) % groups) for source in range(groups)])

    by_sub = rates.T
    slots = []
    for over in range(subs):
        wanted = lax.dynamic_index_in_dim(by_sub, sub ^ over, 0, keepdims=False)
        slots.append(to_sub(wanted, over) if over else wanted)
    slots = jnp.stack(slots)
    rate = jnp.concatenate([lax.dynamic_index_in_dim(slots, sub ^ at, 0, keepdims=False) for at in range(subs)])
    rate = rate.reshape(tokens, 1)

    pieces = spread([keys, values], top)
    for over in order:
        pieces[over] = sent(pieces[over], over)
    query_pieces = spread([queries], 1)
    for over in order:
        query_pieces[over] = sent(query_pieces[over], over)

    halved = top * rows == WINDOW
    if halved:
        links = [(source, source + 1) for source in range(groups - 1)]
        early = []
        for over in range(top):
            late = jnp.where(place >= top, pieces[over], pieces[over + top])
            early.append(lax.ppermute(late, "grp", links))

    parts = groups if FD % (groups * 128) == 0 else 1
    last = [over for over in range(members) if over % top == top - 1]
    most = [over for over in range(members) if over % top != top - 1]

    def updated(overs, given, parts):
        return update_call(which, overs, [pieces[over] for over in overs], rate, given, parts)

    begun = updated(most, (fast_gate, fast_up, fast_down), 0)
    steps = updated(last, begun, parts)

    matrices = (fast_gate, fast_up, fast_down)
    weights = []
    if parts > 1:
        for number, (low, high) in enumerate(SHARES):
            share = steps[number * parts : (number + 1) * parts]
            got = [share[0]] + [to_group(share[ahead], ahead) for ahead in range(1, parts)]
            mine = renorm_call(which, got, matrices[low:high])
            weights.append([mine] + [to_group(mine, ahead) for ahead in range(1, parts)])
    else:
        whole = jnp.stack([sub, sub * 0]).astype(jnp.int32)
        got = [lax.psum(steps[0], "grp") if groups > 1 else steps[0]]
        weights.append([renorm_call(whole, got, matrices)])

    if halved:
        attended = attention_call(which, query_pieces, pieces, [], None, 1)
        attended = attention_call(which, query_pieces, pieces, early, attended, 0)
    else:
        key, value = arrange_call(which, pieces)
        (query,) = arrange_call(which, query_pieces)
        early_key = from_earlier(key)
        early_value = from_earlier(value)
        attended = short_attention(group, query, early_key, key, early_value, value)

    slots = [None] * subs
    gain = lax.dynamic_slice_in_dim(out_gain, sub * FD, FD).reshape(1, FD)
    for over in range(subs - 1, -1, -1):
        block = (sub ^ over).astype(jnp.int32)[None]
        chosen = query_pieces[over * halves : (over + 1) * halves]
        mixed = readout_call(which, block, chosen, weights, attended, gain)
        slots[over] = to_sub(mixed, over) if over else mixed
    if subs == 1:
        return slots[0]
    out = None
    for overs in ((0, 1), *((over,) for over in range(subs - 1, 1, -1))):
        out = join_call(which, overs, [slots[over] for over in overs], out, subs)
    return out


def join_body(which, *rest, overs):
    slots, (out_ref, sems) = rest[: len(overs)], rest[-2:]
    copies = []
    for number, over in enumerate(overs):
        at = pl.multiple_of(lax.bitwise_xor(which[0], over) * FD, FD)
        copies.append(pltpu.make_async_copy(slots[number], out_ref.at[:, pl.ds(at, FD)], sems.at[number]))
        copies[-1].start()
    for copy in copies:
        copy.wait()


def join_call(which, overs, slots, out, subs):
    raw = pl.BlockSpec(memory_space=pltpu.HBM)
    given = list(slots) if out is None else [*slots, out]
    return pl.pallas_call(
        functools.partial(join_body, overs=overs),
        out_shape=jax.ShapeDtypeStruct((slots[0].shape[0], FD * subs), bf16),
        grid_spec=pltpu.PrefetchScalarGridSpec(
            num_scalar_prefetch=1,
            grid=(1,),
            in_specs=[LOCAL] * len(slots) + [raw] * (len(given) - len(slots)),
            out_specs=raw,
            scratch_shapes=[pltpu.SemaphoreType.DMA((len(slots),))],
        ),
        input_output_aliases={} if out is None else {1 + len(slots): 0},
        compiler_params=pltpu.CompilerParams(vmem_limit_bytes=6 << 20),
        name="join",
    )(which, *given)


def short_body(group_ref, q_ref, kp_ref, kc_ref, vp_ref, vc_ref, out_ref):
    rows, before = q_ref.shape[0], kp_ref.shape[0]
    factor = 1.0 / math.sqrt(AHD)
    query = q_ref[...]
    at = lax.broadcasted_iota(jnp.int32, (rows, before), 0)
    back = lax.broadcasted_iota(jnp.int32, (rows, before), 1)
    score_p = dot(query, kp_ref[...], NT) * factor
    score_p = jnp.where((back > at) & (back >= before - group_ref[0] * rows), score_p, -1e30)
    own = lax.broadcasted_iota(jnp.int32, (rows, rows), 1) <= lax.broadcasted_iota(jnp.int32, (rows, rows), 0)
    score_c = jnp.where(own, dot(query, kc_ref[...], NT) * factor, -1e30)
    peak = jnp.maximum(jnp.max(score_p, axis=-1, keepdims=True), jnp.max(score_c, axis=-1, keepdims=True))
    expo_p, expo_c = jnp.exp(score_p - peak), jnp.exp(score_c - peak)
    total = jnp.sum(expo_p, axis=-1, keepdims=True) + jnp.sum(expo_c, axis=-1, keepdims=True)
    result = dot(expo_p.astype(bf16), vp_ref[...], NN) + dot(expo_c.astype(bf16), vc_ref[...], NN)
    out_ref[...] = result / total


def short_attention(group, q, kp, kc, vp, vc):
    tokens, width = q.shape
    here = pl.BlockSpec((tokens, AHD), lambda h, _: (0, h))
    prior = pl.BlockSpec((WINDOW, AHD), lambda h, _: (0, h))
    return pl.pallas_call(
        short_body,
        out_shape=jax.ShapeDtypeStruct((tokens, width), f32),
        grid_spec=pltpu.PrefetchScalarGridSpec(
            num_scalar_prefetch=1,
            grid=(width // AHD,),
            in_specs=[here, prior, here, prior, here],
            out_specs=here,
        ),
        compiler_params=pltpu.CompilerParams(dimension_semantics=("arbitrary",), vmem_limit_bytes=40 << 20),
        name="short_attention",
    )(group.astype(jnp.int32)[None], q, kp, kc, vp, vc)


def solution(mesh):
    contexts, halves = mesh.shape["ctx"], mesh.shape["head"]

    def run(queries, keys, values, rates, fast_gate, fast_up, fast_down, out_gain):
        subs = fast_gate.shape[0] // halves
        split = Mesh(mesh.devices.reshape(contexts // subs, subs, halves), ("grp", "sub", "head"))
        rows = P(("grp", "sub", "head"), None)
        matrix = P("head", None, None)
        step = jax.shard_map(
            planned,
            mesh=split,
            in_specs=(rows, rows, rows, P(("grp", "sub"), "head"), matrix, matrix, matrix, P("head")),
            out_specs=P(("grp", "sub"), "head"),
            check_vma=False,
        )
        return step(queries, keys, values, rates, fast_gate, fast_up, fast_down, out_gain)

    return run
```
